256 devices in a mesh: gz: 64 (over x, y_lo, z), gx: 4 (over y_hi, core).
Axes of the slice: x: 4, y: 4 (y_hi: 2, y_lo: 2; y = y_hi * 2 + y_lo), z: 8, core: 2. Of those that a mesh axis runs over, the one named last changes fastest.
Arguments:
- noisy_volume: float32 [256, 512, 512], P('gz', 'gx'), may hold values from -3 to 3, as said below
- tv_weight: float32 [256, 512, 512], P('gz', 'gx'), may hold values from 0.05 to 0.5
Outputs:
- denoised: float32 [256, 512, 512], P('gz', 'gx')
- gap_values: float32 [4], replicated
- step_values: float32 [4], replicated
The draws below stay inside these ranges and needn't reach their ends.
Inputs may be any that keep to these rules, and one draw needn't show every extreme that they name: `noisy_volume`: voxel intensities.
All inputs are finite; a program needn't handle non-finite values.
Results may differ from the reference program's by a relative error of at most 0.0001.
Values sent between devices are 32-bit elements; how exact they have to be, the bound alone decides.
A program may use at most 64 MiB of HBM per device.

```python
import math
import jax
import jax.numpy as jnp

ITERS = 4
NZ = 256
NX = 512
NY = 512


def draw_noisy_volume(key, part):
    base = jax.random.fold_in(key, 11)
    key_rough = jax.random.fold_in(base, 0)
    position = jnp.arange(NZ, dtype=jnp.float32) / max(NZ - 1, 1)
    rough = jax.random.uniform(key_rough, (NZ, NX, NY), jnp.float32, minval=-1.0, maxval=1.0)
    planes_scale = (3.0 ** position)[:, None, None]
    volume = planes_scale * rough
    return volume.astype(jnp.float32)


def block_scale(own_key, extent, pieces, low, largest):
    gain = 1.0
    for dim, parts in pieces:
        steps = jax.random.uniform(jax.random.fold_in(jax.random.fold_in(own_key, 6), dim), (parts,), jnp.float32, low / len(pieces), largest / len(pieces))
        gain = gain * jnp.repeat(jnp.exp(steps), extent[dim] // parts).reshape((-1,) + (1,) * (len(extent) - 1 - dim))
    return gain


def setup_inputs(seed: int = 0) -> dict:
    keys = jax.random.split(jax.random.key(seed), 3)
    return {
        "noisy_volume": draw_noisy_volume(jax.random.fold_in(keys[2], 71), 0),
        "tv_weight": jnp.clip(jnp.exp(math.log(0.5) - 2.3025851 * jax.random.uniform(keys[1], (NZ, NX, NY), jnp.float32) ** block_scale(keys[1], (NZ, NX, NY), ((0, 64), (1, 4)), -0.2, 0.2)), 0.05, 0.5),
    }


primal_step = 0.28
dual_step = 0.28

def gradient(volume):
    along_z = jnp.concatenate([volume[1:] - volume[:-1], jnp.zeros_like(volume[:1])], axis=0)
    along_x = jnp.concatenate([volume[:, 1:] - volume[:, :-1], jnp.zeros_like(volume[:, :1])], axis=1)
    along_y = jnp.concatenate([volume[:, :, 1:] - volume[:, :, :-1], jnp.zeros_like(volume[:, :, :1])], axis=2)
    return (along_z, along_x, along_y)

def divergence(dual_field):
    dual_z, dual_x, dual_y = dual_field
    back_z = dual_z - jnp.concatenate([jnp.zeros_like(dual_z[:1]), dual_z[:-1]], axis=0)
    back_x = dual_x - jnp.concatenate([jnp.zeros_like(dual_x[:, :1]), dual_x[:, :-1]], axis=1)
    back_y = dual_y - jnp.concatenate([jnp.zeros_like(dual_y[:, :, :1]), dual_y[:, :, :-1]], axis=2)
    return back_z + back_x + back_y

def reference(noisy_volume, tv_weight):
    cell_count = noisy_volume.shape[0] * noisy_volume.shape[1] * noisy_volume.shape[2]
    primal = noisy_volume
    extrapolated = noisy_volume
    zeros_field = jnp.zeros_like(noisy_volume)
    dual_field = (zeros_field, zeros_field, zeros_field)
    gap_list = []
    step_list = []
    for iteration in range(ITERS):
        grad_extra = gradient(extrapolated)
        grad_primal = gradient(primal)
        proposed = tuple((dual_part + dual_step * grad_part for dual_part, grad_part in zip(dual_field, grad_extra)))
        magnitude = jnp.sqrt(proposed[0] * proposed[0] + proposed[1] * proposed[1] + proposed[2] * proposed[2])
        shrink = tv_weight / jnp.maximum(tv_weight, magnitude)
        dual_field = tuple((part * shrink for part in proposed))
        spread = divergence(dual_field)
        updated = (primal + primal_step * (spread + noisy_volume)) / (1.0 + primal_step)
        total_var = jnp.sqrt(grad_primal[0] * grad_primal[0] + grad_primal[1] * grad_primal[1] + grad_primal[2] * grad_primal[2])
        misfit = primal - noisy_volume
        shifted = noisy_volume + spread
        gap_terms = 0.5 * misfit * misfit + tv_weight * total_var - 0.5 * noisy_volume * noisy_volume + 0.5 * shifted * shifted
        gap_list.append(jnp.sum(gap_terms) / cell_count)
        change = updated - primal
        step_list.append(jnp.sqrt(jnp.sum(change * change) / cell_count))
        extrapolated = 2.0 * updated - primal
        primal = updated
    return (primal, jnp.stack(gap_list), jnp.stack(step_list))
```

```python
import jax
import jax.numpy as jnp
from jax import lax
from jax.experimental import pallas as pl
from jax.experimental.pallas import tpu as pltpu
from jax.sharding import PartitionSpec as P

ITERS = 4
PRIMAL = 0.28
DUAL = 0.28
TINY = 1.1754944e-38
F32 = jnp.float32
LANES = 128
RING_Z = 8


def spread_rows(ref, planes, row):
    return jnp.concatenate([ref[z, pl.ds(row, 1), :] for z in planes], axis=0)


def lane_next(parts, lane):
    count = len(parts)
    rolled = [pltpu.roll(part, LANES - 1, 1) for part in parts]
    edge = lane == LANES - 1
    return [
        jnp.where(edge, rolled[m + 1] if m + 1 < count else parts[m], rolled[m]) for m in range(count)
    ]


def lane_prev(parts, lane):
    count = len(parts)
    rolled = [pltpu.roll(part, 1, 1) for part in parts]
    edge = lane == 0
    return [
        jnp.where(edge, rolled[m - 1] if m else jnp.zeros_like(parts[0]), rolled[m])
        for m in range(count)
    ]


def cut(value):
    return [value[:, m * LANES : (m + 1) * LANES] for m in range(value.shape[1] // LANES)]


def project(proposed, weight):
    square = proposed[0] * proposed[0] + proposed[1] * proposed[1] + proposed[2] * proposed[2]
    return jnp.minimum(1.0, weight * lax.rsqrt(jnp.maximum(square, TINY)))


def row_dual(here, above, after, dual, weight, keep):
    lane = lax.broadcasted_iota(jnp.int32, (here.shape[0], LANES), 1)
    here, above, after, weight = cut(here), cut(above), cut(after), cut(weight)
    beside = lane_next(here, lane)
    out = []
    for m in range(len(here)):
        delta = ((above[m] - here[m]) * keep, after[m] - here[m], beside[m] - here[m])
        proposed = [DUAL * d for d in delta]
        if dual is not None:
            proposed = [dual[i][m] + proposed[i] for i in range(3)]
        shrink = project(proposed, weight[m])
        out.append([part * shrink for part in proposed])
    return [jnp.concatenate([out[m][i] for m in range(len(here))], axis=1) for i in range(3)]


def make_kernel(planes, rows, cols, n_gz, n_gx):
    blocks = rows // 8
    chunk_rows = 16
    chunks = rows // chunk_rows
    parts = cols // LANES
    cells = planes * rows * cols * n_gz * n_gx
    top = planes
    half = chunks // 2

    def kernel(
        noisy_hbm, weight_hbm, out_ref, gap_ref, step_ref,
        ub, wt, pz, px, py, uu, rx, rdiag, sx, sdiag, swx, wx, prow, totals, slots,
        load_sem, z_send, z_recv, w_send, w_recv, x_send, x_recv, wx_send, wx_recv, r_send, r_recv,
    ):
        gz, gx = lax.axis_index("gz"), lax.axis_index("gx")
        up, down = lax.rem(gz + 1, n_gz), lax.rem(gz + n_gz - 1, n_gz)
        right, left = lax.rem(gx + 1, n_gx), lax.rem(gx + n_gx - 1, n_gx)
        keep_above = jnp.where(gz == n_gz - 1, 0.0, 1.0).astype(F32)
        keep_below = jnp.where(gz == 0, 0.0, 1.0).astype(F32)
        keep_left = jnp.where(gx == 0, 0.0, 1.0).astype(F32)
        at_right = gx == n_gx - 1

        col, z, yh, core = gz // RING_Z, lax.rem(gz, RING_Z), gx // 2, lax.rem(gx, 2)
        first_id = z * 2 + core
        second_id = col * 2 + yh

        def first_peer(i):
            return {"gz": col * RING_Z + i // 2, "gx": yh * 2 + lax.rem(i, 2)}

        def second_peer(i):
            return {"gz": (i // 2) * RING_Z + z, "gx": lax.rem(i, 2) * 2 + core}

        group = 16

        loads = [
            pltpu.make_async_copy(noisy_hbm, ub.at[0, pl.ds(1, planes), pl.ds(0, rows)], load_sem.at[0]),
            pltpu.make_async_copy(weight_hbm, wt.at[pl.ds(1, planes)], load_sem.at[1]),
        ]
        for load in loads:
            load.start()

        barrier = pltpu.get_barrier_semaphore()
        near = [(up, gx), (down, gx), (gz, right), (gz, left), (up, left), (down, right)]
        for a, b in near:
            pl.semaphore_signal(barrier, 1, device_id={"gz": a, "gx": b}, device_id_type=pl.DeviceIdType.MESH)

        def greet(t, carry):
            for own, peer in ((first_id, first_peer), (second_id, second_peer)):
                other = lax.rem(own + t, group)
                pl.semaphore_signal(barrier, 1, device_id=peer(other), device_id_type=pl.DeviceIdType.MESH)
            return carry

        lax.fori_loop(1, group, greet, 0)
        for load in loads:
            load.wait()

        def remote(src, dst, send, recv, a, b):
            return pltpu.make_async_remote_copy(
                src_ref=src, dst_ref=dst, send_sem=send, recv_sem=recv,
                device_id={"gz": a, "gx": b}, device_id_type=pl.DeviceIdType.MESH,
            )

        def chunk_of(c):
            return pl.ds(pl.multiple_of(c * chunk_rows, chunk_rows), chunk_rows)

        def z_up(k, c):
            return remote(ub.at[k, top, chunk_of(c)], ub.at[k, 0, chunk_of(c)],
                          z_send.at[k, 0, c], z_recv.at[k, 0, c], up, gx)

        def z_down(k, c):
            return remote(ub.at[k, 1, chunk_of(c)], ub.at[k, planes + 1, chunk_of(c)],
                          z_send.at[k, 1, c], z_recv.at[k, 1, c], down, gx)

        def w_up(c):
            return remote(wt.at[top, chunk_of(c)], wt.at[0, chunk_of(c)], w_send.at[c], w_recv.at[c], up, gx)

        def x_copy(k, kind):
            if kind == 0:
                return remote(sx.at[k, 0], rx.at[k, 0], x_send.at[k, 0], x_recv.at[k, 0], gz, right)
            if kind == 1:
                return remote(sx.at[k, 1], rx.at[k, 1], x_send.at[k, 1], x_recv.at[k, 1], gz, left)
            if kind == 2:
                return remote(sdiag.at[k, 0], rdiag.at[k, 0], x_send.at[k, 2], x_recv.at[k, 2], down, right)
            return remote(sdiag.at[k, 1], rdiag.at[k, 1], x_send.at[k, 3], x_recv.at[k, 3], up, left)

        def wx_copy():
            return remote(swx, wx, wx_send, wx_recv, gz, right)

        def stage_last_row(k):
            last = spread_rows(ub.at[k], range(1, planes + 1), rows - 1)
            sx[k, 0] = last
            sdiag[k, 0] = last[:1]

        def stage_first_row(k):
            first = spread_rows(ub.at[k], range(1, planes + 1), 0)
            sx[k, 1] = first
            sdiag[k, 1] = first[planes - 1 :]

        stage_last_row(0)
        stage_first_row(0)
        swx[...] = spread_rows(wt, range(1, planes + 1), rows - 1)

        pl.semaphore_wait(barrier, len(near) + 2 * (group - 1))

        def send_first(j, carry):
            c = lax.rem(half - 1 + j, chunks)
            z_up(0, c).start()
            z_down(0, c).start()
            w_up(c).start()
            return carry

        lax.fori_loop(0, chunks, send_first, 0)
        for kind in range(4):
            x_copy(0, kind).start()
        wx_copy().start()

        lane = lax.broadcasted_iota(jnp.int32, (8, LANES), 1)
        sub = lax.broadcasted_iota(jnp.int32, (8, LANES), 0)
        plane_of = lax.broadcasted_iota(jnp.int32, (planes, LANES), 0)
        keep_rows = jnp.where(plane_of == planes - 1, keep_above, 1.0)

        def lanes(m):
            return pl.ds(m * LANES, LANES)

        def first_halo_row(k):
            x_copy(k, 0).wait_recv()
            x_copy(k, 2).wait_recv()
            if k == 0:
                wx_copy().wait_recv()
            here = rx[k, 0]
            above = jnp.concatenate([here[1:], rdiag[k, 0]], axis=0)
            old = None if k == 0 else [cut(prow[i]) for i in range(3)]
            new = row_dual(here, above, sx[k, 1], old, wx[...], keep_rows)
            for i in range(3):
                prow[i] = new[i]
            along = new[1] * keep_left
            for q in range(planes):
                px[k % 2, q + 1, pl.ds(7, 1), :] = along[q : q + 1]

        def last_halo_row(k):
            x_copy(k, 1).wait_recv()
            x_copy(k, 3).wait_recv()
            for q in range(planes + 1):
                row = rx[k, 1, pl.ds(q - 1, 1), :] if q else rdiag[k, 1]
                own = ub[k, q, pl.ds(rows - 1, 1), :]
                row = jnp.where(at_right, own, row)
                ub[k, q, pl.ds(rows, 1), :] = row
                if k and q:
                    before = ub[0, q, pl.ds(rows, 1), :] if k == 1 else uu[(k - 1) % 2, q, pl.ds(rows, 1), :]
                    uu[k % 2, q, pl.ds(rows, 1), :] = 0.5 * (row + before)

        def start_row(k, s):
            own = range(1, planes + 1)
            here = spread_rows(ub.at[k], own, s - 1)
            above = spread_rows(ub.at[k], range(2, planes + 2), s - 1)
            after = spread_rows(ub.at[k], own, s)
            weight = spread_rows(wt, own, s - 1)
            old = None
            if k:
                was = (k - 1) % 2
                old = [
                    cut(spread_rows(pz.at[was], own, s - 1)),
                    cut(spread_rows(px.at[was], own, s - 1 + 8)),
                    cut(spread_rows(py.at[was], own, s - 1)),
                ]
            new = row_dual(here, above, after, old, weight, keep_rows)
            for q in range(planes):
                px[k % 2, q + 1, pl.ds(s - 1 + 8, 1), :] = new[1][q : q + 1]

        def next_rows(block, row):
            return jnp.where(sub == 7, row, pltpu.roll(block, 7, 0))

        def block_step(k, b, sums):
            r = pl.multiple_of(b * 8, 8)
            here_rows, after_row = pl.ds(r, 8), pl.ds(r + 8, 1)
            was, now = (k - 1) % 2, k % 2
            last = k == ITERS - 1

            def get_u(q, m):
                if k == 0:
                    return ub[0, q, here_rows, lanes(m)]
                return uu[now, q, here_rows, lanes(m)]

            if k:
                for m in range(parts):
                    q = planes + 1
                    before = ub[0, q, here_rows, lanes(m)] if k == 1 else uu[was, q, here_rows, lanes(m)]
                    uu[now, q, here_rows, lanes(m)] = 0.5 * (ub[k, q, here_rows, lanes(m)] + before)

            gap_a = gap_b = step_a = jnp.zeros((8, LANES), F32)
            dual_below = None
            for q in range(planes + 1):
                here = [ub[k, q, here_rows, lanes(m)] for m in range(parts)]
                beside = lane_next(here, lane)
                duals, total_var = [], []
                for m in range(parts):
                    delta_z = ub[k, q + 1, here_rows, lanes(m)] - here[m]
                    if q == planes:
                        delta_z = delta_z * keep_above
                    delta_x = next_rows(here[m], ub[k, q, after_row, lanes(m)]) - here[m]
                    delta_y = beside[m] - here[m]
                    weight = wt[q, here_rows, lanes(m)]
                    proposed = [DUAL * delta_z, DUAL * delta_x, DUAL * delta_y]
                    if k:
                        proposed[0] = pz[was, q, here_rows, lanes(m)] + proposed[0]
                        proposed[1] = px[was, q, pl.ds(r + 8, 8), lanes(m)] + proposed[1]
                        proposed[2] = py[was, q, here_rows, lanes(m)] + proposed[2]
                    shrink = project(proposed, weight)
                    new = [part * shrink for part in proposed]
                    if q == 0:
                        new[0] = new[0] * keep_below
                    duals.append(new)
                    if not last:
                        pz[now, q, here_rows, lanes(m)] = new[0]
                        py[now, q, here_rows, lanes(m)] = new[2]
                    if not last or q:
                        px[now, q, pl.ds(r + 8, 8), lanes(m)] = new[1]
                    if k == 0 and q:
                        square = delta_z * delta_z + delta_x * delta_x + delta_y * delta_y
                        total_var.append(weight * (square * lax.rsqrt(jnp.maximum(square, TINY))))
                if q:
                    if k:
                        value = [get_u(q, m) for m in range(parts)]
                        beside_u = lane_next(value, lane)
                        for m in range(parts):
                            delta_z = get_u(q + 1, m) - value[m]
                            if q == planes:
                                delta_z = delta_z * keep_above
                            delta_x = next_rows(value[m], uu[now, q, after_row, lanes(m)]) - value[m]
                            delta_y = beside_u[m] - value[m]
                            square = delta_z * delta_z + delta_x * delta_x + delta_y * delta_y
                            weight = wt[q, here_rows, lanes(m)]
                            total_var.append(weight * (square * lax.rsqrt(jnp.maximum(square, TINY))))
                    else:
                        value = here
                    before_y = lane_prev([d[2] for d in duals], lane)
                    for m in range(parts):
                        above_x = px[now, q, here_rows, lanes(m)]
                        before_x = pltpu.roll(jnp.where(sub == 7, above_x, duals[m][1]), 1, 0)
                        div = (duals[m][0] - dual_below[m]) + (duals[m][1] - before_x) + (duals[m][2] - before_y[m])
                        noisy = ub[0, q, here_rows, lanes(m)]
                        shifted = noisy + div
                        change = (PRIMAL / (1.0 + PRIMAL)) * (shifted - value[m])
                        updated = value[m] + change
                        terms = div * (shifted + noisy)
                        if k:
                            misfit = value[m] - noisy
                            terms = terms + misfit * misfit
                        gap_a = gap_a + terms
                        gap_b = gap_b + total_var[m]
                        step_a = step_a + change * change
                        if last:
                            out_ref[q - 1, here_rows, lanes(m)] = updated
                        else:
                            uu[(k + 1) % 2, q, here_rows, lanes(m)] = updated
                            ub[k + 1, q, here_rows, lanes(m)] = updated + change
                dual_below = [d[0] for d in duals]
            return (sums[0] + (0.5 * gap_a + gap_b), sums[1] + step_a)

        def wait_chunk(k, c):
            z_up(k, c).wait_recv()
            z_down(k, c).wait_recv()
            if k == 0:
                w_up(c).wait_recv()

        for k in range(ITERS):
            first = half + k
            wait_chunk(k, (first - 1) % chunks)
            wait_chunk(k, first % chunks)
            start_row(k, (first % chunks) * chunk_rows)

            def chunk_step(i, sums, k=k, first=first):
                c = lax.rem(first + i, chunks)

                @pl.when(i < chunks - 2)
                def _():
                    wait_chunk(k, lax.rem(c + 1, chunks))

                @pl.when(c == 0)
                def _():
                    first_halo_row(k)

                @pl.when(c == chunks - 1)
                def _():
                    last_halo_row(k)

                sums = lax.fori_loop(0, 2, lambda j, s: block_step(k, 2 * c + j, s), sums)
                if k < ITERS - 1:
                    z_up(k + 1, c).start()
                    z_down(k + 1, c).start()

                    @pl.when(c == 0)
                    def _():
                        stage_first_row(k + 1)
                        x_copy(k + 1, 1).start()
                        x_copy(k + 1, 3).start()

                    @pl.when(c == chunks - 1)
                    def _():
                        stage_last_row(k + 1)
                        x_copy(k + 1, 0).start()
                        x_copy(k + 1, 2).start()

                return sums

            zero = jnp.zeros((8, LANES), F32)
            gap_sum, step_sum = lax.fori_loop(0, chunks, chunk_step, (zero, zero))
            totals[0, pl.ds(k, 1), :] = jnp.sum(gap_sum, axis=0, keepdims=True)
            totals[0, pl.ds(ITERS + k, 1), :] = jnp.sum(step_sum, axis=0, keepdims=True)

        value = totals[0]
        for stage, (own, peer) in enumerate(((first_id, first_peer), (second_id, second_peer))):
            if stage:
                totals[stage] = value
            slots[stage, own] = value

            def r_copy(slot, other, stage=stage, peer=peer):
                return pltpu.make_async_remote_copy(
                    src_ref=totals.at[stage], dst_ref=slots.at[stage, slot],
                    send_sem=r_send.at[stage, other], recv_sem=r_recv.at[stage, slot],
                    device_id=peer(other), device_id_type=pl.DeviceIdType.MESH,
                )

            def send(t, carry, own=own, r_copy=r_copy):
                r_copy(own, lax.rem(own + t, group)).start()
                return carry

            def receive(t, carry, own=own, r_copy=r_copy):
                other = lax.rem(own + t, group)
                r_copy(other, other).wait_recv()
                return carry

            lax.fori_loop(1, group, send, 0)
            lax.fori_loop(1, group, receive, 0)
            value = slots[stage, 0]
            for i in range(1, group):
                value = value + slots[stage, i]

            def sent(t, carry, own=own, r_copy=r_copy):
                r_copy(own, lax.rem(own + t, group)).wait_send()
                return carry

            if stage:
                done = sent
            else:
                done_first = sent

        mean = jnp.sum(value, axis=1, keepdims=True) / cells
        root = jnp.sqrt(mean)
        for k in range(ITERS):
            gap_ref[k] = mean[k, 0]
            step_ref[k] = root[ITERS + k, 0]

        lax.fori_loop(1, group, done_first, 0)
        lax.fori_loop(1, group, done, 0)

        def drain(c, carry):
            for k in range(ITERS):
                z_up(k, c).wait_send()
                z_down(k, c).wait_send()
            w_up(c).wait_send()
            return carry

        lax.fori_loop(0, chunks, drain, 0)
        for k in range(ITERS):
            for kind in range(4):
                x_copy(k, kind).wait_send()
        wx_copy().wait_send()

    return kernel


def solution(mesh):
    n_gz, n_gx = mesh.shape["gz"], mesh.shape["gx"]

    def shards(noisy, weight):
        planes, rows, cols = noisy.shape
        chunks = rows // 16
        dma = pltpu.SemaphoreType.DMA
        return pl.pallas_call(
            make_kernel(planes, rows, cols, n_gz, n_gx),
            name="tv_steps",
            out_shape=(
                jax.ShapeDtypeStruct(noisy.shape, F32),
                jax.ShapeDtypeStruct((ITERS,), F32),
                jax.ShapeDtypeStruct((ITERS,), F32),
            ),
            in_specs=[pl.BlockSpec(memory_space=pl.ANY)] * 2,
            out_specs=(
                pl.BlockSpec(memory_space=pltpu.VMEM),
                pl.BlockSpec(memory_space=pltpu.SMEM),
                pl.BlockSpec(memory_space=pltpu.SMEM),
            ),
            scratch_shapes=[
                pltpu.VMEM((ITERS, planes + 2, rows + 8, cols), F32),
                pltpu.VMEM((planes + 1, rows, cols), F32),
                pltpu.VMEM((2, planes + 1, rows, cols), F32),
                pltpu.VMEM((2, planes + 1, rows + 8, cols), F32),
                pltpu.VMEM((2, planes + 1, rows, cols), F32),
                pltpu.VMEM((2, planes + 2, rows + 8, cols), F32),
                pltpu.VMEM((ITERS, 2, planes, cols), F32),
                pltpu.VMEM((ITERS, 2, 1, cols), F32),
                pltpu.VMEM((ITERS, 2, planes, cols), F32),
                pltpu.VMEM((ITERS, 2, 1, cols), F32),
                pltpu.VMEM((planes, cols), F32),
                pltpu.VMEM((planes, cols), F32),
                pltpu.VMEM((3, planes, cols), F32),
                pltpu.VMEM((2, 8, LANES), F32),
                pltpu.VMEM((2, 16, 8, LANES), F32),
                dma((2,)),
                dma((ITERS, 2, chunks)),
                dma((ITERS, 2, chunks)),
                dma((chunks,)),
                dma((chunks,)),
                dma((ITERS, 4)),
                dma((ITERS, 4)),
                dma,
                dma,
                dma((2, 16)),
                dma((2, 16)),
            ],
            compiler_params=pltpu.CompilerParams(
                collective_id=0, has_side_effects=True, vmem_limit_bytes=60 * 1024 * 1024
            ),
        )(noisy, weight)

    spec = P("gz", "gx", None)
    return jax.shard_map(
        shards, mesh=mesh, in_specs=(spec, spec), out_specs=(spec, P(), P()), check_vma=False
    )
```

```python
import jax
import jax.numpy as jnp
from jax import lax
from jax.experimental import pallas as pl
from jax.experimental.pallas import tpu as pltpu
from jax.sharding import PartitionSpec as P

ITERS = 4
PRIMAL = 0.28
DUAL = 0.28
TINY = 1.1754944e-38
F32 = jnp.float32
LANES = 128
RING_Z = 8
GROUP = 16
EXT = 8
BLOCK = 8
CHUNK = 16
MESH = pl.DeviceIdType.MESH


def lane_next(parts, lane):
    count = len(parts)
    rolled = [pltpu.roll(part, LANES - 1, 1) for part in parts]
    edge = lane == LANES - 1
    return [
        jnp.where(edge, rolled[m + 1] if m + 1 < count else parts[m], rolled[m]) for m in range(count)
    ]


def lane_prev(parts, lane):
    count = len(parts)
    rolled = [pltpu.roll(part, 1, 1) for part in parts]
    edge = lane == 0
    return [
        jnp.where(edge, rolled[m - 1] if m else jnp.zeros_like(parts[0]), rolled[m])
        for m in range(count)
    ]


def root_inverse(square):
    return lax.rsqrt(jnp.maximum(square, TINY))


def norm2(vector):
    return vector[0] * vector[0] + vector[1] * vector[1] + vector[2] * vector[2]


def make_kernel(planes, rows, cols, n_gz, n_gx):
    parts = cols // LANES
    cells = planes * rows * cols * n_gz * n_gx
    top = planes
    blocks = (rows + 2 * EXT) // BLOCK
    chunks = blocks * BLOCK // CHUNK
    own_first, own_last = 1, blocks - 2

    def kernel(
        noisy_hbm, weight_hbm, out_ref, sums_ref,
        ub, wt, pz, py, uu, px, edges, beside, totals, slots,
        load_sem, z_send, z_recv, w_send, w_recv, x_send, x_recv, r_send, r_recv,
    ):
        gz, gx = lax.axis_index("gz"), lax.axis_index("gx")
        up, down = lax.rem(gz + 1, n_gz), lax.rem(gz + n_gz - 1, n_gz)
        right, left = lax.rem(gx + 1, n_gx), lax.rem(gx + n_gx - 1, n_gx)
        keep_above = jnp.where(gz == n_gz - 1, 0.0, 1.0).astype(F32)
        keep_below = jnp.where(gz == 0, 0.0, 1.0).astype(F32)
        keep_left = jnp.where(gx == 0, 0.0, 1.0).astype(F32)
        keep_right = jnp.where(gx == n_gx - 1, 0.0, 1.0).astype(F32)

        col, z, yh, core = gz // RING_Z, lax.rem(gz, RING_Z), gx // 2, lax.rem(gx, 2)
        first_id = z * 2 + core
        second_id = col * 2 + yh

        def first_peer(i):
            return {"gz": col * RING_Z + i // 2, "gx": yh * 2 + lax.rem(i, 2)}

        def second_peer(i):
            return {"gz": (i // 2) * RING_Z + z, "gx": lax.rem(i, 2) * 2 + core}

        loads = [
            pltpu.make_async_copy(src.at[:, :, pl.ds(m * LANES, LANES)],
                                  dst.at[pl.ds(1, planes), m, pl.ds(EXT, rows)], load_sem.at[i, m])
            for i, (src, dst) in enumerate(((noisy_hbm, ub.at[0]), (weight_hbm, wt)))
            for m in range(parts)
        ]
        for load in loads:
            load.start()

        barrier = pltpu.get_barrier_semaphore()
        near = [(up, gx), (down, gx), (gz, right), (gz, left)]
        for a, b in near:
            pl.semaphore_signal(barrier, 1, device_id={"gz": a, "gx": b}, device_id_type=MESH)

        def greet(t, carry):
            for own, peer in ((first_id, first_peer), (second_id, second_peer)):
                pl.semaphore_signal(barrier, 1, device_id=peer(lax.rem(own + t, GROUP)), device_id_type=MESH)
            return carry

        lax.fori_loop(1, GROUP, greet, 0)
        for load in loads:
            load.wait()

        def remote(src, dst, send, recv, a, b):
            return pltpu.make_async_remote_copy(
                src_ref=src, dst_ref=dst, send_sem=send, recv_sem=recv,
                device_id={"gz": a, "gx": b}, device_id_type=MESH,
            )

        def chunk_rows(k, c):
            if isinstance(c, int) and c in (0, chunks - 1):
                margin = ITERS - k
                if c == 0:
                    return pl.ds(EXT - margin, CHUNK - EXT + margin)
                return pl.ds(c * CHUNK, CHUNK - EXT + margin)
            return pl.ds(pl.multiple_of(c * CHUNK, CHUNK), CHUNK)

        def z_up(k, c):
            at = chunk_rows(k, c)
            return remote(ub.at[k, top, :, at], ub.at[k, 0, :, at], z_send.at[k, 0, c], z_recv.at[k, 0, c], up, gx)

        def z_down(k, c):
            at = chunk_rows(k, c)
            return remote(ub.at[k, 1, :, at], ub.at[k, top + 1, :, at], z_send.at[k, 1, c], z_recv.at[k, 1, c], down, gx)

        def w_up(c):
            at = chunk_rows(0, c)
            return remote(wt.at[top, :, at], wt.at[0, :, at], w_send.at[c], w_recv.at[c], up, gx)

        own_planes = pl.ds(1, planes)
        arrays = (ub.at[0, own_planes], wt.at[own_planes])
        x_copies = []
        for i, (source, to, side) in enumerate(((EXT + rows - ITERS, EXT - ITERS, right), (EXT, EXT + rows, left))):
            for n, array in enumerate(arrays):
                edges[i, n] = array[:, :, pl.ds(source, ITERS), :]
                x_copies.append(remote(edges.at[i, n], beside.at[i, n], x_send.at[i, n], x_recv.at[i, n], gz, side))

        pl.semaphore_wait(barrier, len(near) + 2 * (GROUP - 1))
        for copy in x_copies:
            copy.start()

        def receive_x(i):
            to = (EXT - ITERS, EXT + rows)[i]
            for n, array in enumerate(arrays):
                x_copies[2 * i + n].wait_recv()
                array[:, :, pl.ds(to, ITERS), :] = beside[i, n]

        def send_first(c):
            z_up(0, c).start()
            w_up(c).start()
            z_down(0, c).start()

        def send_loop(c, carry):
            send_first(c)
            return carry

        for copy in x_copies:
            copy.wait_send()
        receive_x(0)
        send_first(0)
        receive_x(1)
        lax.fori_loop(1, chunks - 1, send_loop, 0)
        send_first(chunks - 1)

        lane = lax.broadcasted_iota(jnp.int32, (BLOCK, LANES), 1)
        sub = lax.broadcasted_iota(jnp.int32, (BLOCK, LANES), 0)
        keep_last_row = jnp.where(sub == BLOCK - 1, keep_right, 1.0)

        def get_u(k, q, m, at):
            return ub[0, q, m, at, :] if k == 0 else uu[k % 2, q, m, at, :]

        def block_step(k, j, sums, place="own"):
            r = j * BLOCK if isinstance(j, int) else pl.multiple_of(j * BLOCK, BLOCK)
            at, at_next = pl.ds(r, BLOCK), pl.ds(r + 1, BLOCK)
            at_x, at_before_x = pl.ds(r + BLOCK, BLOCK), pl.ds(r + BLOCK - 1, BLOCK)
            was, now = (k - 1) % 2, k % 2
            last = k == ITERS - 1
            counted = place in ("own", "last")
            update = counted or not last

            if k:
                for m in range(parts):
                    new = (0.5 / DUAL) * ub[k, top + 1, m, at, :] + 0.5 * get_u(k - 1, top + 1, m, at)
                    uu[now, top + 1, m, at, :] = new

            gap_a = gap_b = step_a = jnp.zeros((BLOCK, LANES), F32)
            dual_below = None
            for q in range(planes + 1):
                here = [ub[k, q, m, at, :] for m in range(parts)]
                beside = lane_next(here, lane)
                duals, total_var = [], []
                for m in range(parts):
                    delta = [ub[k, q + 1, m, at, :] - here[m], ub[k, q, m, at_next, :] - here[m], beside[m] - here[m]]
                    if q == top:
                        delta[0] = delta[0] * keep_above
                    if place == "last":
                        delta[1] = delta[1] * keep_last_row
                    weight = wt[q, m, at, :]
                    if k:
                        proposed = [
                            pz[was, q, m, at, :] + delta[0],
                            px[was, q, m, at_x, :] + delta[1],
                            py[was, q, m, at, :] + delta[2],
                        ]
                    else:
                        proposed = [DUAL * part for part in delta]
                    shrink = jnp.minimum(1.0, weight * root_inverse(norm2(proposed)))
                    new = [part * shrink for part in proposed]
                    if q == 0:
                        new[0] = new[0] * keep_below
                    if place == "first":
                        new[1] = new[1] * keep_left
                    duals.append(new)
                    if not last:
                        pz[now, q, m, at, :] = new[0]
                        py[now, q, m, at, :] = new[2]
                    if not last or q:
                        px[now, q, m, at_x, :] = new[1]
                    if k == 0 and q and counted:
                        square = norm2(delta)
                        total_var.append(weight * (square * root_inverse(square)))
                if q and update:
                    value = here if k == 0 else [get_u(k, q, m, at) for m in range(parts)]
                    if k and counted:
                        beside_u = lane_next(value, lane)
                        for m in range(parts):
                            delta = [
                                get_u(k, q + 1, m, at) - value[m],
                                get_u(k, q, m, at_next) - value[m],
                                beside_u[m] - value[m],
                            ]
                            if q == top:
                                delta[0] = delta[0] * keep_above
                            if place == "last":
                                delta[1] = delta[1] * keep_last_row
                            square = norm2(delta)
                            total_var.append(wt[q, m, at, :] * (square * root_inverse(square)))
                    before_y = lane_prev([d[2] for d in duals], lane)
                    for m in range(parts):
                        before_x = px[now, q, m, at_before_x, :]
                        div = (duals[m][0] - dual_below[m]) + (duals[m][1] - before_x) + (duals[m][2] - before_y[m])
                        noisy = ub[0, q, m, at, :]
                        shifted = noisy + div
                        change = (PRIMAL / (1.0 + PRIMAL)) * (shifted - value[m])
                        updated = value[m] + change
                        if counted:
                            terms = div * (shifted + noisy)
                            if k:
                                misfit = value[m] - noisy
                                terms = terms + misfit * misfit
                            gap_a = gap_a + terms
                            gap_b = gap_b + total_var[m]
                            step_a = step_a + change * change
                        if last:
                            out_ref[q - 1, pl.ds(r - EXT, BLOCK), pl.ds(m * LANES, LANES)] = updated
                        else:
                            uu[(k + 1) % 2, q, m, at, :] = updated
                            ub[k + 1, q, m, at, :] = DUAL * (updated + change)
                dual_below = [d[0] for d in duals]
            if not counted:
                return sums
            return (sums[0] + (0.5 * gap_a + gap_b), sums[1] + step_a)

        def send_chunk(k, c):
            if k < ITERS - 1:
                z_up(k + 1, c).start()
                z_down(k + 1, c).start()

        def wait_up(k, c):
            z_up(k, c).wait_recv()
            if k == 0:
                w_up(c).wait_recv()

        for k in range(ITERS):
            zero = jnp.zeros((BLOCK, LANES), F32)
            sums = (zero, zero)
            wait_up(k, 0)
            z_down(k, 0).wait_recv()
            wait_up(k, 1)
            sums = block_step(k, 0, sums, "first")
            sums = block_step(k, 1, sums)
            send_chunk(k, 0)

            def chunk_step(c, sums, k=k):
                z_down(k, c).wait_recv()

                @pl.when(c < chunks - 2)
                def _():
                    wait_up(k, c + 1)

                @pl.when(c == chunks - 2)
                def _():
                    wait_up(k, chunks - 1)

                sums = lax.fori_loop(0, CHUNK // BLOCK, lambda i, s: block_step(k, 2 * c + i, s), sums)
                send_chunk(k, c)
                return sums

            sums = lax.fori_loop(1, chunks - 1, chunk_step, sums)
            z_down(k, chunks - 1).wait_recv()
            sums = block_step(k, own_last, sums, "last")
            if k < ITERS - 1:
                block_step(k, own_last + 1, sums, "after")
            send_chunk(k, chunks - 1)
            totals[0, pl.ds(k, 1), :] = jnp.sum(sums[0], axis=0, keepdims=True)
            totals[0, pl.ds(ITERS + k, 1), :] = jnp.sum(sums[1], axis=0, keepdims=True)

        by_row = jnp.sum(totals[0], axis=1, keepdims=True)
        value = jnp.sum(jnp.where(lane == sub, by_row, 0.0), axis=0, keepdims=True)
        done = []
        for stage, (mine, peer) in enumerate(((first_id, first_peer), (second_id, second_peer))):
            slots[stage, mine] = value
            totals[1 + stage, pl.ds(0, 1), :] = value

            def r_copy(slot, other, stage=stage, peer=peer):
                return pltpu.make_async_remote_copy(
                    src_ref=totals.at[1 + stage, pl.ds(0, 1)], dst_ref=slots.at[stage, slot],
                    send_sem=r_send.at[stage, other], recv_sem=r_recv.at[stage, slot],
                    device_id=peer(other), device_id_type=MESH,
                )

            def send(t, carry, mine=mine, r_copy=r_copy):
                r_copy(mine, lax.rem(mine + t, GROUP)).start()
                return carry

            def receive(t, carry, mine=mine, r_copy=r_copy):
                other = lax.rem(mine + t, GROUP)
                r_copy(other, other).wait_recv()
                return carry

            def sent(t, carry, mine=mine, r_copy=r_copy):
                r_copy(mine, lax.rem(mine + t, GROUP)).wait_send()
                return carry

            lax.fori_loop(1, GROUP, send, 0)
            lax.fori_loop(1, GROUP, receive, 0)
            value = slots[stage, 0]
            for i in range(1, GROUP):
                value = value + slots[stage, i]
            done.append(sent)

        mean = value / cells
        sums_ref[...] = jnp.where(lane[:1] < ITERS, mean, jnp.sqrt(mean))

        for sent in done:
            lax.fori_loop(1, GROUP, sent, 0)

        def drain(c):
            for k in range(ITERS):
                z_up(k, c).wait_send()
                z_down(k, c).wait_send()
            w_up(c).wait_send()

        def drain_loop(c, carry):
            drain(c)
            return carry

        drain(0)
        lax.fori_loop(1, chunks - 1, drain_loop, 0)
        drain(chunks - 1)

    return kernel


def solution(mesh):
    n_gz, n_gx = mesh.shape["gz"], mesh.shape["gx"]

    def shards(noisy, weight):
        planes, rows, cols = noisy.shape
        parts = cols // LANES
        chunks = (rows + 2 * EXT) // CHUNK
        tall = rows + 3 * EXT
        dma = pltpu.SemaphoreType.DMA
        denoised, sums = pl.pallas_call(
            make_kernel(planes, rows, cols, n_gz, n_gx),
            name="tv_steps",
            out_shape=(
                pltpu.VMEM(noisy.shape, F32),
                pltpu.VMEM((1, LANES), F32),
            ),
            in_specs=[pl.BlockSpec(memory_space=pl.ANY)] * 2,
            out_specs=(
                pl.BlockSpec(memory_space=pltpu.VMEM),
                pl.BlockSpec(memory_space=pltpu.VMEM),
            ),
            scratch_shapes=[
                pltpu.VMEM((ITERS, planes + 2, parts, tall, LANES), F32),
                pltpu.VMEM((planes + 1, parts, tall, LANES), F32),
                pltpu.VMEM((2, planes + 1, parts, tall, LANES), F32),
                pltpu.VMEM((2, planes + 1, parts, tall, LANES), F32),
                pltpu.VMEM((2, planes + 2, parts, tall, LANES), F32),
                pltpu.VMEM((2, planes + 1, parts, tall + 2 * EXT, LANES), F32),
                pltpu.VMEM((2, 2, planes, parts, ITERS, LANES), F32),
                pltpu.VMEM((2, 2, planes, parts, ITERS, LANES), F32),
                pltpu.VMEM((3, 8, LANES), F32),
                pltpu.VMEM((2, GROUP, 1, LANES), F32),
                dma((2, parts)),
                dma((ITERS, 2, chunks)),
                dma((ITERS, 2, chunks)),
                dma((chunks,)),
                dma((chunks,)),
                dma((2, 2)),
                dma((2, 2)),
                dma((2, GROUP)),
                dma((2, GROUP)),
            ],
            compiler_params=pltpu.CompilerParams(
                collective_id=0, has_side_effects=True, vmem_limit_bytes=60 * 1024 * 1024
            ),
        )(noisy, weight)
        return denoised, sums[0, :ITERS], sums[0, ITERS : 2 * ITERS]

    spec = P("gz", "gx", None)
    return jax.shard_map(
        shards, mesh=mesh, in_specs=(spec, spec), out_specs=(spec, P(), P()), check_vma=False
    )
```

```python
import jax
import jax.numpy as jnp
from jax import lax
from jax.experimental import pallas as pl
from jax.experimental.pallas import tpu as pltpu
from jax.sharding import PartitionSpec as P

ITERS = 4
PRIMAL = 0.28
DUAL = 0.28
TINY = 1.1754944e-38
F32 = jnp.float32
LANES = 128
RING_Z = 8
GROUP = 16
EXT = 8
BLOCK = 8
CHUNK = 16
MESH = pl.DeviceIdType.MESH


def lane_next(parts, lane):
    count = len(parts)
    rolled = [pltpu.roll(part, LANES - 1, 1) for part in parts]
    edge = lane == LANES - 1
    return [
        jnp.where(edge, rolled[m + 1] if m + 1 < count else parts[m], rolled[m]) for m in range(count)
    ]


def lane_prev(parts, lane):
    count = len(parts)
    rolled = [pltpu.roll(part, 1, 1) for part in parts]
    edge = lane == 0
    return [
        jnp.where(edge, rolled[m - 1] if m else jnp.zeros_like(parts[0]), rolled[m])
        for m in range(count)
    ]


def root_inverse(square):
    return lax.rsqrt(jnp.maximum(square, TINY))


def norm2(vector):
    return vector[0] * vector[0] + vector[1] * vector[1] + vector[2] * vector[2]


def make_kernel(planes, rows, cols, n_gz, n_gx):
    parts = cols // LANES
    cells = planes * rows * cols * n_gz * n_gx
    top = planes
    blocks = (rows + 2 * EXT) // BLOCK
    chunks = blocks * BLOCK // CHUNK
    own_first, own_last = 1, blocks - 2

    def kernel(
        noisy_hbm, weight_hbm, out_ref, sums_ref,
        ub, wt, pz, py, uu, px, edges, beside, totals, slots,
        load_sem, z_send, z_recv, w_send, w_recv, x_send, x_recv, r_send, r_recv,
    ):
        gz, gx = lax.axis_index("gz"), lax.axis_index("gx")
        up, down = lax.rem(gz + 1, n_gz), lax.rem(gz + n_gz - 1, n_gz)
        right, left = lax.rem(gx + 1, n_gx), lax.rem(gx + n_gx - 1, n_gx)
        keep_above = jnp.where(gz == n_gz - 1, 0.0, 1.0).astype(F32)
        keep_below = jnp.where(gz == 0, 0.0, 1.0).astype(F32)
        keep_left = jnp.where(gx == 0, 0.0, 1.0).astype(F32)
        keep_right = jnp.where(gx == n_gx - 1, 0.0, 1.0).astype(F32)

        col, z, yh, core = gz // RING_Z, lax.rem(gz, RING_Z), gx // 2, lax.rem(gx, 2)
        first_id = z * 2 + core
        second_id = col * 2 + yh

        def first_peer(i):
            return {"gz": col * RING_Z + i // 2, "gx": yh * 2 + lax.rem(i, 2)}

        def second_peer(i):
            return {"gz": (i // 2) * RING_Z + z, "gx": lax.rem(i, 2) * 2 + core}

        loads = [
            pltpu.make_async_copy(src.at[:, :, pl.ds(m * LANES, LANES)],
                                  dst.at[pl.ds(1, planes), m, pl.ds(EXT, rows)], load_sem.at[i, m])
            for i, (src, dst) in enumerate(((noisy_hbm, ub.at[0]), (weight_hbm, wt)))
            for m in range(parts)
        ]
        for load in loads:
            load.start()

        barrier = pltpu.get_barrier_semaphore()
        near = [(up, gx), (down, gx), (gz, right), (gz, left)]
        for a, b in near:
            pl.semaphore_signal(barrier, 1, device_id={"gz": a, "gx": b}, device_id_type=MESH)

        def greet(t, carry):
            for own, peer in ((first_id, first_peer), (second_id, second_peer)):
                pl.semaphore_signal(barrier, 1, device_id=peer(lax.rem(own + t, GROUP)), device_id_type=MESH)
            return carry

        lax.fori_loop(1, GROUP, greet, 0)
        for load in loads:
            load.wait()

        def remote(src, dst, send, recv, a, b):
            return pltpu.make_async_remote_copy(
                src_ref=src, dst_ref=dst, send_sem=send, recv_sem=recv,
                device_id={"gz": a, "gx": b}, device_id_type=MESH,
            )

        def chunk_rows(k, c):
            if isinstance(c, int) and c in (0, chunks - 1):
                margin = ITERS - k
                if c == 0:
                    return pl.ds(EXT - margin, CHUNK - EXT + margin)
                return pl.ds(c * CHUNK, CHUNK - EXT + margin)
            return pl.ds(pl.multiple_of(c * CHUNK, CHUNK), CHUNK)

        def z_up(k, c):
            at = chunk_rows(k, c)
            return remote(ub.at[k, top, :, at], ub.at[k, 0, :, at], z_send.at[k, 0, c], z_recv.at[k, 0, c], up, gx)

        def z_down(k, c):
            at = chunk_rows(k, c)
            return remote(ub.at[k, 1, :, at], ub.at[k, top + 1, :, at], z_send.at[k, 1, c], z_recv.at[k, 1, c], down, gx)

        def w_up(c):
            at = chunk_rows(0, c)
            return remote(wt.at[top, :, at], wt.at[0, :, at], w_send.at[c], w_recv.at[c], up, gx)

        own_planes = pl.ds(1, planes)
        arrays = (ub.at[0, own_planes], wt.at[own_planes])
        x_copies = []
        for i, (source, to, side) in enumerate(((EXT + rows - ITERS, EXT - ITERS, right), (EXT, EXT + rows, left))):
            for n, array in enumerate(arrays):
                edges[i, n] = array[:, :, pl.ds(source, ITERS), :]
                x_copies.append(remote(edges.at[i, n], beside.at[i, n], x_send.at[i, n], x_recv.at[i, n], gz, side))

        pl.semaphore_wait(barrier, len(near) + 2 * (GROUP - 1))
        for copy in x_copies:
            copy.start()

        def receive_x(i):
            to = (EXT - ITERS, EXT + rows)[i]
            for n, array in enumerate(arrays):
                x_copies[2 * i + n].wait_recv()
                array[:, :, pl.ds(to, ITERS), :] = beside[i, n]

        def send_first(c):
            z_up(0, c).start()
            w_up(c).start()
            z_down(0, c).start()

        def send_loop(c, carry):
            send_first(c)
            return carry

        for copy in x_copies:
            copy.wait_send()
        send_first(1)
        receive_x(0)
        send_first(0)
        receive_x(1)
        lax.fori_loop(2, chunks - 1, send_loop, 0)
        send_first(chunks - 1)

        lane = lax.broadcasted_iota(jnp.int32, (BLOCK, LANES), 1)
        sub = lax.broadcasted_iota(jnp.int32, (BLOCK, LANES), 0)
        keep_last_row = jnp.where(sub == BLOCK - 1, keep_right, 1.0)

        def get_u(k, q, m, at):
            return ub[0, q, m, at, :] if k == 0 else uu[k % 2, q, m, at, :]

        def block_step(k, j, sums, place="own"):
            r = j * BLOCK if isinstance(j, int) else pl.multiple_of(j * BLOCK, BLOCK)
            at, at_next = pl.ds(r, BLOCK), pl.ds(r + 1, BLOCK)
            at_x, at_before_x = pl.ds(r + BLOCK, BLOCK), pl.ds(r + BLOCK - 1, BLOCK)
            was, now = (k - 1) % 2, k % 2
            last = k == ITERS - 1
            counted = place in ("own", "last")
            update = counted or not last

            if k:
                for m in range(parts):
                    new = (0.5 / DUAL) * ub[k, top + 1, m, at, :] + 0.5 * get_u(k - 1, top + 1, m, at)
                    uu[now, top + 1, m, at, :] = new

            gap_a = gap_b = step_a = jnp.zeros((BLOCK, LANES), F32)
            dual_below = None
            for q in range(planes + 1):
                here = [ub[k, q, m, at, :] for m in range(parts)]
                beside = lane_next(here, lane)
                duals, total_var = [], []
                for m in range(parts):
                    delta = [ub[k, q + 1, m, at, :] - here[m], ub[k, q, m, at_next, :] - here[m], beside[m] - here[m]]
                    if q == top:
                        delta[0] = delta[0] * keep_above
                    if place == "last":
                        delta[1] = delta[1] * keep_last_row
                    weight = wt[q, m, at, :]
                    if k:
                        proposed = [
                            pz[was, q, m, at, :] + delta[0],
                            px[was, q, m, at_x, :] + delta[1],
                            py[was, q, m, at, :] + delta[2],
                        ]
                    else:
                        proposed = [DUAL * part for part in delta]
                    shrink = jnp.minimum(1.0, weight * root_inverse(norm2(proposed)))
                    new = [part * shrink for part in proposed]
                    if q == 0:
                        new[0] = new[0] * keep_below
                    if place == "first":
                        new[1] = new[1] * keep_left
                    duals.append(new)
                    if not last:
                        pz[now, q, m, at, :] = new[0]
                        py[now, q, m, at, :] = new[2]
                    if not last or q:
                        px[now, q, m, at_x, :] = new[1]
                    if k == 0 and q and counted:
                        square = norm2(delta)
                        total_var.append(weight * (square * root_inverse(square)))
                if q and update:
                    value = here if k == 0 else [get_u(k, q, m, at) for m in range(parts)]
                    if k and counted:
                        beside_u = lane_next(value, lane)
                        for m in range(parts):
                            delta = [
                                get_u(k, q + 1, m, at) - value[m],
                                get_u(k, q, m, at_next) - value[m],
                                beside_u[m] - value[m],
                            ]
                            if q == top:
                                delta[0] = delta[0] * keep_above
                            if place == "last":
                                delta[1] = delta[1] * keep_last_row
                            square = norm2(delta)
                            total_var.append(wt[q, m, at, :] * (square * root_inverse(square)))
                    before_y = lane_prev([d[2] for d in duals], lane)
                    for m in range(parts):
                        before_x = px[now, q, m, at_before_x, :]
                        div = (duals[m][0] - dual_below[m]) + (duals[m][1] - before_x) + (duals[m][2] - before_y[m])
                        noisy = ub[0, q, m, at, :]
                        shifted = noisy + div
                        change = (PRIMAL / (1.0 + PRIMAL)) * (shifted - value[m])
                        updated = value[m] + change
                        if counted:
                            terms = div * (shifted + noisy)
                            if k:
                                misfit = value[m] - noisy
                                terms = terms + misfit * misfit
                            gap_a = gap_a + terms
                            gap_b = gap_b + total_var[m]
                            step_a = step_a + change * change
                        if last:
                            out_ref[q - 1, pl.ds(r - EXT, BLOCK), pl.ds(m * LANES, LANES)] = updated
                        else:
                            uu[(k + 1) % 2, q, m, at, :] = updated
                            ub[k + 1, q, m, at, :] = DUAL * (updated + change)
                dual_below = [d[0] for d in duals]
            if not counted:
                return sums
            return (sums[0] + (0.5 * gap_a + gap_b), sums[1] + step_a)

        def send_chunk(k, c):
            if k < ITERS - 1:
                z_up(k + 1, c).start()
                z_down(k + 1, c).start()

        def wait_up(k, c):
            z_up(k, c).wait_recv()
            if k == 0:
                w_up(c).wait_recv()

        for k in range(ITERS):
            zero = jnp.zeros((BLOCK, LANES), F32)
            sums = (zero, zero)
            wait_up(k, 0)
            z_down(k, 0).wait_recv()
            wait_up(k, 1)
            sums = block_step(k, 0, sums, "first")
            sums = block_step(k, 1, sums)
            send_chunk(k, 0)

            def chunk_step(c, sums, k=k):
                z_down(k, c).wait_recv()

                @pl.when(c < chunks - 2)
                def _():
                    wait_up(k, c + 1)

                @pl.when(c == chunks - 2)
                def _():
                    wait_up(k, chunks - 1)

                sums = lax.fori_loop(0, CHUNK // BLOCK, lambda i, s: block_step(k, 2 * c + i, s), sums)
                send_chunk(k, c)
                return sums

            sums = lax.fori_loop(1, chunks - 1, chunk_step, sums)
            z_down(k, chunks - 1).wait_recv()
            sums = block_step(k, own_last, sums, "last")
            if k < ITERS - 1:
                block_step(k, own_last + 1, sums, "after")
            send_chunk(k, chunks - 1)
            totals[0, pl.ds(k, 1), :] = jnp.sum(sums[0], axis=0, keepdims=True)
            totals[0, pl.ds(ITERS + k, 1), :] = jnp.sum(sums[1], axis=0, keepdims=True)

        def drain(c):
            for k in range(ITERS):
                z_up(k, c).wait_send()
                z_down(k, c).wait_send()
            w_up(c).wait_send()

        def drain_loop(c, carry):
            drain(c)
            return carry

        def drain_all():
            drain(0)
            lax.fori_loop(1, chunks - 1, drain_loop, 0)
            drain(chunks - 1)

        by_row = jnp.sum(totals[0], axis=1, keepdims=True)
        value = jnp.sum(jnp.where(lane == sub, by_row, 0.0), axis=0, keepdims=True)
        for stage, (mine, peer) in enumerate(((first_id, first_peer), (second_id, second_peer))):
            slots[stage, mine] = value
            totals[1 + stage, pl.ds(0, 1), :] = value

            def r_copy(slot, other, stage=stage, peer=peer):
                return pltpu.make_async_remote_copy(
                    src_ref=totals.at[1 + stage, pl.ds(0, 1)], dst_ref=slots.at[stage, slot],
                    send_sem=r_send.at[stage, other], recv_sem=r_recv.at[stage, slot],
                    device_id=peer(other), device_id_type=MESH,
                )

            def send(t, carry, mine=mine, r_copy=r_copy):
                r_copy(mine, lax.rem(mine + t, GROUP)).start()
                return carry

            def receive(t, carry, mine=mine, r_copy=r_copy):
                other = lax.rem(mine + t, GROUP)
                r_copy(other, other).wait_recv()
                return carry

            def sent(t, carry, mine=mine, r_copy=r_copy):
                r_copy(mine, lax.rem(mine + t, GROUP)).wait_send()
                return carry

            for t in range(1, GROUP):
                send(t, 0)
            if stage == 0:
                drain_all()
            lax.fori_loop(1, GROUP, sent, 0)
            lax.fori_loop(1, GROUP, receive, 0)
            value = slots[stage, 0]
            for i in range(1, GROUP):
                value = value + slots[stage, i]

        mean = value / cells
        sums_ref[...] = jnp.where(lane[:1] < ITERS, mean, jnp.sqrt(mean))

    return kernel


def solution(mesh):
    n_gz, n_gx = mesh.shape["gz"], mesh.shape["gx"]

    def shards(noisy, weight):
        planes, rows, cols = noisy.shape
        parts = cols // LANES
        chunks = (rows + 2 * EXT) // CHUNK
        tall = rows + 3 * EXT
        dma = pltpu.SemaphoreType.DMA
        denoised, sums = pl.pallas_call(
            make_kernel(planes, rows, cols, n_gz, n_gx),
            name="tv_steps",
            out_shape=(
                pltpu.VMEM(noisy.shape, F32),
                pltpu.VMEM((1, LANES), F32),
            ),
            in_specs=[pl.BlockSpec(memory_space=pl.ANY)] * 2,
            out_specs=(
                pl.BlockSpec(memory_space=pltpu.VMEM),
                pl.BlockSpec(memory_space=pltpu.VMEM),
            ),
            scratch_shapes=[
                pltpu.VMEM((ITERS, planes + 2, parts, tall, LANES), F32),
                pltpu.VMEM((planes + 1, parts, tall, LANES), F32),
                pltpu.VMEM((2, planes + 1, parts, tall, LANES), F32),
                pltpu.VMEM((2, planes + 1, parts, tall, LANES), F32),
                pltpu.VMEM((2, planes + 2, parts, tall, LANES), F32),
                pltpu.VMEM((2, planes + 1, parts, tall + 2 * EXT, LANES), F32),
                pltpu.VMEM((2, 2, planes, parts, ITERS, LANES), F32),
                pltpu.VMEM((2, 2, planes, parts, ITERS, LANES), F32),
                pltpu.VMEM((3, 8, LANES), F32),
                pltpu.VMEM((2, GROUP, 1, LANES), F32),
                dma((2, parts)),
                dma((ITERS, 2, chunks)),
                dma((ITERS, 2, chunks)),
                dma((chunks,)),
                dma((chunks,)),
                dma((2, 2)),
                dma((2, 2)),
                dma((2, GROUP)),
                dma((2, GROUP)),
            ],
            compiler_params=pltpu.CompilerParams(
                collective_id=0, has_side_effects=True, vmem_limit_bytes=60 * 1024 * 1024
            ),
        )(noisy, weight)
        return denoised, sums[0, :ITERS], sums[0, ITERS : 2 * ITERS]

    spec = P("gz", "gx", None)
    return jax.shard_map(
        shards, mesh=mesh, in_specs=(spec, spec), out_specs=(spec, P(), P()), check_vma=False
    )
```

```python
import jax
import jax.numpy as jnp
from jax import lax
from jax.experimental import pallas as pl
from jax.experimental.pallas import tpu as pltpu
from jax.sharding import PartitionSpec as P

ITERS = 4
PRIMAL = 0.28
DUAL = 0.28
TINY = 1.1754944e-38
F32 = jnp.float32
LANES = 128
RING_Z = 8
GROUP = 16
EXT = 8
BLOCK = 8
CHUNK = 16
EARLY = 16
MESH = pl.DeviceIdType.MESH


def lane_next(parts, lane):
    count = len(parts)
    rolled = [pltpu.roll(part, LANES - 1, 1) for part in parts]
    edge = lane == LANES - 1
    return [
        jnp.where(edge, rolled[m + 1] if m + 1 < count else parts[m], rolled[m]) for m in range(count)
    ]


def lane_prev(parts, lane):
    count = len(parts)
    rolled = [pltpu.roll(part, 1, 1) for part in parts]
    edge = lane == 0
    return [
        jnp.where(edge, rolled[m - 1] if m else jnp.zeros_like(parts[0]), rolled[m])
        for m in range(count)
    ]


def root_inverse(square):
    return lax.rsqrt(jnp.maximum(square, TINY))


def norm2(vector):
    return vector[0] * vector[0] + vector[1] * vector[1] + vector[2] * vector[2]


def make_kernel(planes, rows, cols, n_gz, n_gx):
    parts = cols // LANES
    cells = planes * rows * cols * n_gz * n_gx
    top = planes
    blocks = (rows + 2 * EXT) // BLOCK
    chunks = blocks * BLOCK // CHUNK
    own_last = blocks - 2
    per_chunk = CHUNK // BLOCK
    inner_end = own_last // per_chunk

    def kernel(
        noisy_hbm, weight_hbm, out_ref, sums_ref,
        ub, wt, pz, py, uu, px, edges, beside, totals, slots,
        load_sem, z_send, z_recv, w_send, w_recv, x_send, x_recv, r_send, r_recv,
    ):
        gz, gx = lax.axis_index("gz"), lax.axis_index("gx")
        up, down = lax.rem(gz + 1, n_gz), lax.rem(gz + n_gz - 1, n_gz)
        right, left = lax.rem(gx + 1, n_gx), lax.rem(gx + n_gx - 1, n_gx)
        keep_above = jnp.where(gz == n_gz - 1, 0.0, 1.0).astype(F32)
        keep_below = jnp.where(gz == 0, 0.0, 1.0).astype(F32)
        keep_left = jnp.where(gx == 0, 0.0, 1.0).astype(F32)
        keep_right = jnp.where(gx == n_gx - 1, 0.0, 1.0).astype(F32)

        col, z, yh, core = gz // RING_Z, lax.rem(gz, RING_Z), gx // 2, lax.rem(gx, 2)
        first_id = z * 2 + core
        second_id = col * 2 + yh

        def first_peer(i):
            return {"gz": col * RING_Z + i // 2, "gx": yh * 2 + lax.rem(i, 2)}

        def second_peer(i):
            return {"gz": (i // 2) * RING_Z + z, "gx": lax.rem(i, 2) * 2 + core}

        loads = [
            pltpu.make_async_copy(src.at[:, :, pl.ds(m * LANES, LANES)],
                                  dst.at[pl.ds(1, planes), m, pl.ds(EXT, rows)], load_sem.at[i, m])
            for i, (src, dst) in enumerate(((noisy_hbm, ub.at[0]), (weight_hbm, wt)))
            for m in range(parts)
        ]
        for load in loads:
            load.start()

        barrier = pltpu.get_barrier_semaphore()
        near = [(up, gx), (down, gx), (gz, right), (gz, left)]
        for a, b in near:
            pl.semaphore_signal(barrier, 1, device_id={"gz": a, "gx": b}, device_id_type=MESH)

        def greet(t, carry):
            for own, peer in ((first_id, first_peer), (second_id, second_peer)):
                pl.semaphore_signal(barrier, 1, device_id=peer(lax.rem(own + t, GROUP)), device_id_type=MESH)
            return carry

        lax.fori_loop(1, GROUP, greet, 0)
        for load in loads:
            load.wait()

        def remote(src, dst, send, recv, a, b):
            return pltpu.make_async_remote_copy(
                src_ref=src, dst_ref=dst, send_sem=send, recv_sem=recv,
                device_id={"gz": a, "gx": b}, device_id_type=MESH,
            )

        def chunk_rows(k, c):
            if isinstance(c, int) and c in (0, chunks - 1):
                margin = ITERS - k
                if c == 0:
                    return pl.ds(EXT - margin, CHUNK - EXT + margin)
                return pl.ds(c * CHUNK, CHUNK - EXT + margin)
            return pl.ds(pl.multiple_of(c * CHUNK, CHUNK), CHUNK)

        def z_up(k, c):
            at = chunk_rows(k, c)
            return remote(ub.at[k, top, :, at], ub.at[k, 0, :, at], z_send.at[k, 0, c], z_recv.at[k, 0, c], up, gx)

        def z_down(k, c):
            at = chunk_rows(k, c)
            return remote(ub.at[k, 1, :, at], ub.at[k, top + 1, :, at], z_send.at[k, 1, c], z_recv.at[k, 1, c], down, gx)

        def w_up(c):
            at = chunk_rows(0, c)
            return remote(wt.at[top, :, at], wt.at[0, :, at], w_send.at[c], w_recv.at[c], up, gx)

        own_planes = pl.ds(1, planes)
        arrays = (ub.at[0, own_planes], wt.at[own_planes])
        x_copies = []
        for i, (source, to, side) in enumerate(((EXT + rows - ITERS, EXT - ITERS, right), (EXT, EXT + rows, left))):
            for n, array in enumerate(arrays):
                edges[i, n] = array[:, :, pl.ds(source, ITERS), :]
            x_copies.append(remote(edges.at[i], beside.at[i], x_send.at[i], x_recv.at[i], gz, side))

        pl.semaphore_wait(barrier, len(near) + 2 * (GROUP - 1))
        for copy in x_copies:
            copy.start()

        def receive_x(i):
            to = (EXT - ITERS, EXT + rows)[i]
            x_copies[i].wait_recv()
            for n, array in enumerate(arrays):
                array[:, :, pl.ds(to, ITERS), :] = beside[i, n]

        def send_first(c):
            z_up(0, c).start()
            w_up(c).start()
            z_down(0, c).start()

        def send_loop(c, carry):
            send_first(c)
            return carry

        for copy in x_copies:
            copy.wait_send()
        early = jnp.where(jnp.logical_or(z == 0, z == RING_Z - 1), 1, 3)
        lax.fori_loop(1, 1 + early, send_loop, 0)
        receive_x(0)
        send_first(0)
        receive_x(1)
        lax.fori_loop(1 + early, chunks - 1, send_loop, 0)
        send_first(chunks - 1)

        lane = lax.broadcasted_iota(jnp.int32, (BLOCK, LANES), 1)
        sub = lax.broadcasted_iota(jnp.int32, (BLOCK, LANES), 0)
        keep_last_row = jnp.where(sub == BLOCK - 1, keep_right, 1.0)

        def get_u(k, q, m, at):
            return ub[0, q, m, at, :] if k == 0 else uu[k % 2, q, m, at, :]

        def block_step(k, j, sums, place="own"):
            r = j * BLOCK if isinstance(j, int) else pl.multiple_of(j * BLOCK, BLOCK)
            at, at_next = pl.ds(r, BLOCK), pl.ds(r + 1, BLOCK)
            at_x, at_before_x = pl.ds(r + BLOCK, BLOCK), pl.ds(r + BLOCK - 1, BLOCK)
            was, now = (k - 1) % 2, k % 2
            last = k == ITERS - 1
            counted = place in ("own", "last")
            update = counted or not last

            if k:
                for m in range(parts):
                    new = (0.5 / DUAL) * ub[k, top + 1, m, at, :] + 0.5 * get_u(k - 1, top + 1, m, at)
                    uu[now, top + 1, m, at, :] = new

            gap_a = gap_b = step_a = jnp.zeros((BLOCK, LANES), F32)
            dual_below = None
            for q in range(planes + 1):
                here = [ub[k, q, m, at, :] for m in range(parts)]
                beside = lane_next(here, lane)
                duals, total_var = [], []
                for m in range(parts):
                    delta = [ub[k, q + 1, m, at, :] - here[m], ub[k, q, m, at_next, :] - here[m], beside[m] - here[m]]
                    if q == top:
                        delta[0] = delta[0] * keep_above
                    if place == "last":
                        delta[1] = delta[1] * keep_last_row
                    weight = wt[q, m, at, :]
                    if k:
                        proposed = [
                            pz[was, q, m, at, :] + delta[0],
                            px[was, q, m, at_x, :] + delta[1],
                            py[was, q, m, at, :] + delta[2],
                        ]
                    else:
                        proposed = [DUAL * part for part in delta]
                    shrink = jnp.minimum(1.0, weight * root_inverse(norm2(proposed)))
                    new = [part * shrink for part in proposed]
                    if q == 0:
                        new[0] = new[0] * keep_below
                    if place == "first":
                        new[1] = new[1] * keep_left
                    duals.append(new)
                    if not last:
                        pz[now, q, m, at, :] = new[0]
                        py[now, q, m, at, :] = new[2]
                    if not last or q:
                        px[now, q, m, at_x, :] = new[1]
                    if k == 0 and q and counted:
                        square = norm2(delta)
                        total_var.append(weight * (square * root_inverse(square)))
                if q and update:
                    value = here if k == 0 else [get_u(k, q, m, at) for m in range(parts)]
                    if k and counted:
                        beside_u = lane_next(value, lane)
                        for m in range(parts):
                            delta = [
                                get_u(k, q + 1, m, at) - value[m],
                                get_u(k, q, m, at_next) - value[m],
                                beside_u[m] - value[m],
                            ]
                            if q == top:
                                delta[0] = delta[0] * keep_above
                            if place == "last":
                                delta[1] = delta[1] * keep_last_row
                            square = norm2(delta)
                            total_var.append(wt[q, m, at, :] * (square * root_inverse(square)))
                    before_y = lane_prev([d[2] for d in duals], lane)
                    for m in range(parts):
                        before_x = px[now, q, m, at_before_x, :]
                        div = (duals[m][0] - dual_below[m]) + (duals[m][1] - before_x) + (duals[m][2] - before_y[m])
                        noisy = ub[0, q, m, at, :]
                        shifted = noisy + div
                        change = (PRIMAL / (1.0 + PRIMAL)) * (shifted - value[m])
                        updated = value[m] + change
                        if counted:
                            terms = div * (shifted + noisy)
                            if k:
                                misfit = value[m] - noisy
                                terms = terms + misfit * misfit
                            gap_a = gap_a + terms
                            gap_b = gap_b + total_var[m]
                            step_a = step_a + change * change
                        if last:
                            out_ref[q - 1, pl.ds(r - EXT, BLOCK), pl.ds(m * LANES, LANES)] = updated
                        else:
                            uu[(k + 1) % 2, q, m, at, :] = updated
                            ub[k + 1, q, m, at, :] = DUAL * (updated + change)
                dual_below = [d[0] for d in duals]
            if not counted:
                return sums
            return (sums[0] + (0.5 * gap_a + gap_b), sums[1] + step_a)

        def send_chunk(k, c):
            if k < ITERS - 1:
                z_up(k + 1, c).start()
                z_down(k + 1, c).start()

        def wait_up(k, c):
            z_up(k, c).wait_recv()
            if k == 0:
                w_up(c).wait_recv()

        for k in range(ITERS):
            zero = jnp.zeros((BLOCK, LANES), F32)
            sums = (zero, zero)
            def edge_chunk(c, sums, k=k):
                z_down(k, c).wait_recv()
                if c + 1 < chunks:
                    wait_up(k, c + 1)
                for j in range(c * per_chunk, (c + 1) * per_chunk):
                    place = {0: "first", own_last: "last", own_last + 1: "after"}.get(j, "own")
                    if place != "after" or k < ITERS - 1:
                        sums = block_step(k, j, sums, place)
                send_chunk(k, c)
                return sums

            def chunk_step(c, sums, k=k):
                z_down(k, c).wait_recv()

                @pl.when(c < inner_end - 1)
                def _():
                    wait_up(k, c + 1)

                @pl.when(c == inner_end - 1)
                def _():
                    wait_up(k, inner_end)

                if per_chunk == 1:
                    sums = block_step(k, c, sums)
                else:
                    sums = lax.fori_loop(0, per_chunk, lambda i, s: block_step(k, per_chunk * c + i, s), sums)
                send_chunk(k, c)
                return sums

            wait_up(k, 0)
            sums = edge_chunk(0, sums)
            sums = lax.fori_loop(1, inner_end, chunk_step, sums)
            for c in range(inner_end, chunks):
                sums = edge_chunk(c, sums)
            totals[0, pl.ds(k, 1), :] = jnp.sum(sums[0], axis=0, keepdims=True)
            totals[0, pl.ds(ITERS + k, 1), :] = jnp.sum(sums[1], axis=0, keepdims=True)

        def drain(c):
            for k in range(ITERS):
                z_up(k, c).wait_send()
                z_down(k, c).wait_send()
            w_up(c).wait_send()

        def drain_loop(c, carry):
            drain(c)
            return carry

        def drain_all():
            drain(0)
            lax.fori_loop(1, chunks - 1, drain_loop, 0)
            drain(chunks - 1)

        by_row = jnp.sum(totals[0], axis=1, keepdims=True)
        value = jnp.sum(jnp.where(lane == sub, by_row, 0.0), axis=0, keepdims=True)
        for stage, (mine, peer) in enumerate(((first_id, first_peer), (second_id, second_peer))):
            slots[stage, mine] = value
            totals[1 + stage, pl.ds(0, 1), :] = value

            def r_copy(slot, other, stage=stage, peer=peer):
                return pltpu.make_async_remote_copy(
                    src_ref=totals.at[1 + stage, pl.ds(0, 1)], dst_ref=slots.at[stage, slot],
                    send_sem=r_send.at[stage, other], recv_sem=r_recv.at[stage, slot],
                    device_id=peer(other), device_id_type=MESH,
                )

            def send(t, carry, mine=mine, r_copy=r_copy):
                r_copy(mine, lax.rem(mine + t, GROUP)).start()
                return carry

            def receive(t, carry, mine=mine, r_copy=r_copy):
                other = lax.rem(mine + t, GROUP)
                r_copy(other, other).wait_recv()
                return carry

            def sent(t, carry, mine=mine, r_copy=r_copy):
                r_copy(mine, lax.rem(mine + t, GROUP)).wait_send()
                return carry

            for t in range(1, GROUP):
                send(t, 0)
            if stage == 0:
                drain_all()
            lax.fori_loop(1, GROUP, sent, 0)
            lax.fori_loop(1, GROUP, receive, 0)
            value = slots[stage, 0]
            for i in range(1, GROUP):
                value = value + slots[stage, i]

        mean = value / cells
        sums_ref[...] = jnp.where(lane[:1] < ITERS, mean, jnp.sqrt(mean))

    return kernel


def solution(mesh):
    n_gz, n_gx = mesh.shape["gz"], mesh.shape["gx"]

    def shards(noisy, weight):
        planes, rows, cols = noisy.shape
        parts = cols // LANES
        chunks = (rows + 2 * EXT) // CHUNK
        tall = rows + 3 * EXT
        dma = pltpu.SemaphoreType.DMA
        denoised, sums = pl.pallas_call(
            make_kernel(planes, rows, cols, n_gz, n_gx),
            name="tv_steps",
            out_shape=(
                pltpu.VMEM(noisy.shape, F32),
                pltpu.VMEM((1, LANES), F32),
            ),
            in_specs=[pl.BlockSpec(memory_space=pl.ANY)] * 2,
            out_specs=(
                pl.BlockSpec(memory_space=pltpu.VMEM),
                pl.BlockSpec(memory_space=pltpu.VMEM),
            ),
            scratch_shapes=[
                pltpu.VMEM((ITERS, planes + 2, parts, tall, LANES), F32),
                pltpu.VMEM((planes + 1, parts, tall, LANES), F32),
                pltpu.VMEM((2, planes + 1, parts, tall, LANES), F32),
                pltpu.VMEM((2, planes + 1, parts, tall, LANES), F32),
                pltpu.VMEM((2, planes + 2, parts, tall, LANES), F32),
                pltpu.VMEM((2, planes + 1, parts, tall + 2 * EXT, LANES), F32),
                pltpu.VMEM((2, 2, planes, parts, ITERS, LANES), F32),
                pltpu.VMEM((2, 2, planes, parts, ITERS, LANES), F32),
                pltpu.VMEM((3, 8, LANES), F32),
                pltpu.VMEM((2, GROUP, 1, LANES), F32),
                dma((2, parts)),
                dma((ITERS, 2, chunks)),
                dma((ITERS, 2, chunks)),
                dma((chunks,)),
                dma((chunks,)),
                dma((2,)),
                dma((2,)),
                dma((2, GROUP)),
                dma((2, GROUP)),
            ],
            compiler_params=pltpu.CompilerParams(
                collective_id=0, has_side_effects=True, vmem_limit_bytes=60 * 1024 * 1024
            ),
        )(noisy, weight)
        return denoised, sums[0, :ITERS], sums[0, ITERS : 2 * ITERS]

    spec = P("gz", "gx", None)
    return jax.shard_map(
        shards, mesh=mesh, in_specs=(spec, spec), out_specs=(spec, P(), P()), check_vma=False
    )
```
